128 devices in a mesh: dom: 128 (over y, z, x, core).
Axes of the slice: x: 4, y: 4, z: 4, core: 2. Of those that a mesh axis runs over, the one named last changes fastest.
Arguments:
- right_side: float32 [131072, 3], P('dom'), may hold values from -10 to 10
- fine_diagonal: float32 [131072, 3], P('dom'), may hold values from 2 to 4
- fine_columns: int32 [131072, 27], P('dom'), may hold values from 0 to 131071, as said below
- fine_blocks: float32 [131072, 27, 3, 3], P('dom'), may hold values from -0.625 to 0.625
- aggregate_of_node: int32 [131072], P('dom'), may hold values from 0 to 31, as said below
- coarse_row_of_aggregate: int32 [4096], P('dom'), may hold values from 0 to 4095, as said below
- coarse_diagonal: float32 [4096, 3], P('dom'), may hold values from 2 to 4
- coarse_columns: int32 [4096, 27], P('dom'), may hold values from 0 to 4095
- coarse_blocks: float32 [4096, 27, 3, 3], P('dom'), may hold values from -0.625 to 0.625
Outputs:
- solution: float32 [131072, 3], P('dom')
- correction: float32 [4096, 3], P('dom')
The draws below stay inside these ranges and needn't reach their ends.
Inputs may be any that keep to these rules, and one draw needn't show every extreme that they name: Every entry of fine_columns differs from its row number by at most 256, and some entry by exactly 256. `aggregate_of_node`: on each device every aggregate number 0 to 31 is used by at least one of its nodes. coarse_row_of_aggregate is a permutation of 0 to 4095; among the 32 aggregates of one device (an aligned block of entries) at most 8 get rows of any one owner, and exactly 8 for some owner.
All inputs are finite; a program needn't handle non-finite values.
Results may differ from the reference program's by a relative error of at most 0.0003.
Values sent between devices are 32-bit elements.
A program may use at most 64 MiB of HBM per device.

```python
import jax
import jax.numpy as jnp
from jax import lax

NODE_DEV = 1024
CAP = 8
WIN = 256
NNZ = 27
CNNZ = 27
SWEEPS = 2
CSWEEPS = 6
AGG_DEV = 32
NODES = 131072
AGGS = 4096


def draw_fine_columns(key, part):
    row_ids = jnp.arange(NODES, dtype=jnp.int32)[:, None]
    offset = jax.random.randint(jax.random.fold_in(key, 13), (NODES, NNZ), -WIN, WIN + 1)
    columns = jnp.clip(row_ids + offset, 0, NODES - 1)
    return columns.at[0, 0].set(WIN).astype(jnp.int32)


def draw_aggregate_of_node(key, part):
    devices = NODES // NODE_DEV
    key_raw, key_mix = jax.random.split(jax.random.fold_in(key, 11))
    labels_raw = jax.random.randint(key_raw, (devices, NODE_DEV), 0, AGG_DEV)
    labels_raw = labels_raw.at[:, :AGG_DEV].set(jnp.arange(AGG_DEV, dtype=jnp.int32)[None, :])
    mixers = jax.random.split(key_mix, devices)
    shuffles = jax.vmap(lambda one_key: jax.random.permutation(one_key, NODE_DEV))(mixers)
    return jnp.take_along_axis(labels_raw, shuffles, axis=1).reshape(-1).astype(jnp.int32)


def draw_coarse_row_of_aggregate(key, part):
    devices = AGGS // AGG_DEV
    groups = AGG_DEV // CAP
    key_group, key_slot, key_label = jax.random.split(jax.random.fold_in(key, 17), 3)
    scores = jax.random.permutation(key_group, devices).astype(jnp.int32)
    scores = scores.at[devices // 2].set(-3).at[1].set(-2).at[devices - 1].set(-1)
    offsets = jnp.argsort(scores, stable=True)[:groups].astype(jnp.int32)
    sources = jnp.arange(devices, dtype=jnp.int32)[:, None]
    label_mix = jax.vmap(lambda one_key: jax.random.permutation(one_key, AGG_DEV))(jax.random.split(key_label, devices)).astype(jnp.int32)
    group_ids = label_mix // CAP
    owners = (sources + offsets[group_ids]) % devices
    within = group_ids * CAP + label_mix % CAP
    slot_mix = jax.vmap(lambda one_key: jax.random.permutation(one_key, AGG_DEV))(jax.random.split(key_slot, devices)).astype(jnp.int32)
    slots = slot_mix[owners, within]
    return (owners * AGG_DEV + slots).reshape(-1).astype(jnp.int32)


def with_ends(drawn, own_key, low, high):
    spot = [jax.random.randint(jax.random.fold_in(own_key, axis), (), 0, length) for axis, length in enumerate(drawn.shape)]
    main_axis = drawn.shape.index(max(drawn.shape))
    neighbour = spot[:main_axis] + [(spot[main_axis] + 1) % drawn.shape[main_axis]] + spot[main_axis + 1:]
    return drawn.at[tuple(spot)].set(low).at[tuple(neighbour)].set(high)


def level_of(own_key, extent, cuts, low, high):
    loudness, own = 1.0, jax.random.fold_in(own_key, 6)
    for dim, blocks in cuts:
        draws = jnp.exp(jax.random.uniform(jax.random.fold_in(own, dim), (blocks,), jnp.float32, low / len(cuts), high / len(cuts)))
        loudness = loudness * jnp.repeat(draws, extent[dim] // blocks).reshape([-1 if axis == dim else 1 for axis in range(len(extent))])
    return loudness


def bell_draw(key, shape, scale, reach, cuts=(), kind=jnp.bfloat16):
    gain = level_of(key, shape, cuts, -0.22, 0.18) if cuts else 1.0
    values = jax.random.normal(key, shape, jnp.float32) * scale * gain
    return jnp.minimum(jnp.maximum(values, -reach), reach).astype(kind)


def setup_inputs(seed: int = 0) -> dict:
    seeds = jax.random.split(jax.random.key(seed), 10)
    return {
        "right_side": bell_draw(seeds[0], (NODES, 3), 2.0, 10.0, ((0, 128),), jnp.float32),
        "fine_diagonal": jnp.clip(2.0 + 2.0 * jax.random.uniform(seeds[1], (NODES, 3), jnp.float32) ** level_of(seeds[1], (NODES, 3), ((0, 128),), -0.2, 0.2), 2.0, 4.0),
        "fine_columns": draw_fine_columns(jax.random.fold_in(seeds[9], 71), 0),
        "fine_blocks": bell_draw(seeds[3], (NODES, NNZ, 3, 3), (3 * NNZ) ** -0.5, 0.625, ((0, 128),), jnp.float32),
        "aggregate_of_node": draw_aggregate_of_node(jax.random.fold_in(seeds[9], 71), 0),
        "coarse_row_of_aggregate": draw_coarse_row_of_aggregate(jax.random.fold_in(seeds[9], 71), 0),
        "coarse_diagonal": jnp.clip(2.0 + 2.0 * jax.random.uniform(seeds[6], (AGGS, 3), jnp.float32) ** level_of(seeds[6], (AGGS, 3), ((0, 128),), -0.2, 0.2), 2.0, 4.0),
        "coarse_columns": with_ends(jax.random.randint(seeds[7], (AGGS, CNNZ), 0, AGGS), jax.random.fold_in(seeds[7], 1), 0, AGGS - 1).astype(jnp.int32),
        "coarse_blocks": bell_draw(seeds[8], (AGGS, CNNZ, 3, 3), (3 * CNNZ) ** -0.5, 0.625, ((0, 128),), jnp.float32),
    }


damping = 0.7


def apply_level(field, diagonal, columns, blocks):
    nearby = field[columns]
    pulled = jnp.einsum("rkij,rkj->ri", blocks, nearby, precision=lax.Precision.HIGHEST)
    return diagonal * field - pulled


def reference(right_side, fine_diagonal, fine_columns, fine_blocks, aggregate_of_node, coarse_row_of_aggregate, coarse_diagonal, coarse_columns, coarse_blocks):
    solution = jnp.zeros_like(right_side)
    for sweep in range(SWEEPS):
        solution = solution + damping * (right_side - apply_level(solution, fine_diagonal, fine_columns, fine_blocks)) / fine_diagonal
    residual = right_side - apply_level(solution, fine_diagonal, fine_columns, fine_blocks)
    node_ids = jnp.arange(NODES, dtype=jnp.int32)
    labels = (node_ids // NODE_DEV) * AGG_DEV + aggregate_of_node
    coarse_rows = coarse_row_of_aggregate[labels]
    coarse_rhs = jax.ops.segment_sum(residual, coarse_rows, num_segments=AGGS)
    correction = jnp.zeros_like(coarse_rhs)
    for sweep in range(CSWEEPS):
        correction = correction + damping * (coarse_rhs - apply_level(correction, coarse_diagonal, coarse_columns, coarse_blocks)) / coarse_diagonal
    solution = solution + correction[coarse_rows]
    for sweep in range(SWEEPS):
        solution = solution + damping * (right_side - apply_level(solution, fine_diagonal, fine_columns, fine_blocks)) / fine_diagonal
    return solution, correction
```

```python
import jax
import jax.numpy as jnp
from jax import lax
from jax.experimental import pallas as pl
from jax.experimental.pallas import tpu as pltpu
from jax.sharding import PartitionSpec as P

MESH = pl.DeviceIdType.MESH
LANES = 128
WIN = 256
CSWEEPS = 6
NEAR_BITS = (1, 2, 8, 32)
FAR_BITS = (4, 16, 64)
damping = 0.7


def subsets(bits):
    masks = [0]
    for bit in bits:
        masks = masks + [mask ^ bit for mask in masks]
    return sorted(masks[1:], key=lambda mask: -bin(mask).count("1"))


NEAR = subsets(NEAR_BITS)
FAR = subsets(FAR_BITS)
MEMBERS, BLOCKS = len(NEAR) + 1, len(FAR) + 1


def bit(value, position):
    return (value >> position) & 1


def member_of(device):
    return (device & 3) | (bit(device, 3) << 2) | (bit(device, 5) << 3)


def block_of(device):
    return bit(device, 2) | (bit(device, 4) << 1) | (bit(device, 6) << 2)


def place_of(row):
    device = row >> 5
    return (member_of(device) << 8) | (block_of(device) << 5) | (row & 31)


def pick(source, lane):
    return jnp.take_along_axis(source, lane, axis=1, mode="promise_in_bounds")


def spread(row, shape=(8, LANES)):
    return jnp.broadcast_to(row, shape)


def iota(shape, axis):
    return lax.broadcasted_iota(jnp.int32, shape, axis)


def kernel(
    right_ref, diagonal_ref, column_ref, block_ref, label_ref, own_ref, cdiagonal_ref, ccolumn_ref, cblock_ref,
    out_ref, correction_ref,
    right, diagonal, place, field, pulled, halo_out, halo_in, halo_new, node_place,
    before, aside, far_table, far_sums, near_table, coarse_block, coarse_place, inverse_chunk, inverse_lane, rhs, tile,
    halo_send, halo_recv, far_send, far_recv, near_send, near_recv,
):
    me = lax.axis_index("dom")
    devices = lax.axis_size("dom")
    member, block = member_of(me), block_of(me)
    after_me, before_me = lax.rem(me + 1, devices), lax.rem(me + devices - 1, devices)
    zero = jnp.zeros((8, LANES), jnp.float32)
    sub, lanes = iota((8, LANES), 0), iota((8, LANES), 1)

    barrier = pltpu.get_barrier_semaphore()
    for mask in FAR + NEAR:
        pl.semaphore_signal(barrier, inc=1, device_id=(me ^ mask,), device_id_type=MESH)
    for neighbour in (after_me, before_me):
        pl.semaphore_signal(barrier, inc=1, device_id=(neighbour,), device_id_type=MESH)

    def remote(source, target, send, recv, device):
        return pltpu.make_async_remote_copy(
            src_ref=source, dst_ref=target, send_sem=send, recv_sem=recv, device_id=(device,), device_id_type=MESH
        )

    def halo_copies(step):
        return [
            remote(halo_out.at[step, 0], halo_in.at[step, 0], halo_send.at[step, 0], halo_recv.at[step, 0], after_me),
            remote(halo_out.at[step, 1], halo_in.at[step, 1], halo_send.at[step, 1], halo_recv.at[step, 1], before_me),
        ]

    def send_halo(step, values):
        for c in range(3):
            halo_out[step, 0, 2 * c : 2 * c + 2, :] = values[c][6:8]
            halo_out[step, 1, 2 * c : 2 * c + 2, :] = values[c][0:2]
        if step == 0:
            halo_out[step, 0, 6:8, :] = node_place[6:8, :]
            halo_out[step, 1, 6:8, :] = node_place[0:2, :]
        else:
            halo_out[step, 0, 6:8, :] = zero[0:2]
            halo_out[step, 1, 6:8, :] = zero[0:2]
        for copy in halo_copies(step):
            copy.start()

    def wait_halo(step):
        for copy in halo_copies(step):
            copy.wait_recv()

    def send_near(step):
        own = near_table.at[step, member]
        for mask in NEAR:
            remote(own, own, near_send.at[step], near_recv.at[step], me ^ mask).start()

    def wait_near(step, sems):
        whole = near_table.at[step, pl.ds(0, MEMBERS - 1)]
        pltpu.make_async_copy(whole, whole, sems.at[step]).wait()

    def send_far(own, index):
        for mask in FAR:
            remote(own, own, far_send.at[index], far_recv.at[index], me ^ mask).start()

    def wait_far(table, index, sems):
        whole = table.at[pl.ds(0, BLOCKS - 1)]
        pltpu.make_async_copy(whole, whole, sems.at[index]).wait()

    for c in range(3):
        for j in range(8):
            span = slice(j * LANES, (j + 1) * LANES)
            right[c, j : j + 1, :] = right_ref[c : c + 1, span]
            diagonal[c, j : j + 1, :] = diagonal_ref[c : c + 1, span]
    own_place = place_of(own_ref[...])
    aside[...] = jnp.zeros((16, LANES), jnp.float32)
    aside[8:9, 0:32] = own_place.astype(jnp.float32)
    node_place[...] = pick(spread(aside[8:9, :]), label_ref[...])
    state = [damping * right[c] / diagonal[c] for c in range(3)]
    for c in range(3):
        field[c] = state[c]

    pl.semaphore_wait(barrier, len(FAR) + len(NEAR) + 2)
    send_halo(0, state)

    before[...] = jnp.zeros(before.shape, jnp.float32)
    for i in range(3):
        for c in range(3):
            q = 3 * i + c
            before[32 * q : 32 * q + 32, 0:27] = cblock_ref[i, c]
    before[288:320, 0:27] = place_of(ccolumn_ref[...]).astype(jnp.float32)
    aside[0:3, 0:32] = cdiagonal_ref[...]
    own_block = far_table.at[block]
    for group in range(3):
        turned = before[128 * group : 128 * group + 128, :].T
        own_block[32 * group : 32 * group + 32, :] = turned[0:32, :]
    extra = pltpu.roll(aside[0:8, :], 64, 1) + pltpu.roll(aside[8:16, :], 96, 1)
    own_block[64:72, :] = own_block[64:72, :] + extra
    send_far(own_block, 0)

    place[24:32, :] = jnp.zeros((8, 8 * LANES), jnp.int32)
    for j in range(8):
        span = slice(j * LANES, (j + 1) * LANES)
        start = me * (8 * LANES) + (j * LANES - WIN)
        for k in range(4):
            rows = slice(8 * k, min(8 * k + 8, 27))
            place[rows, span] = column_ref[rows, span] - start

    def apply_fine(low, high):
        for j in range(8):
            span = slice(j * LANES, (j + 1) * LANES)
            source = []
            for c in range(3):
                line = []
                for t in range(5):
                    at = j + t
                    if at < 2:
                        line.append(low[2 * c + at : 2 * c + at + 1, :])
                    elif at < 10:
                        line.append(field[c, at - 2 : at - 1, :])
                    else:
                        line.append(high[2 * c + at - 10 : 2 * c + at - 9, :])
                source.append(line)
            total = [None] * 3
            tail = [None] * 3
            for k in range(4):
                where = place[8 * k : 8 * k + 8, span]
                lane, chunk = where & (LANES - 1), where >> 7
                masks = [chunk == t for t in range(1, 5)]
                for c in range(3):
                    near = pick(spread(source[c][0]), lane)
                    for t in range(1, 5):
                        near = jnp.where(masks[t - 1], pick(spread(source[c][t]), lane), near)
                    for i in range(3):
                        if k < 3:
                            term = block_ref[i, c, 8 * k : 8 * k + 8, span] * near
                            total[i] = term if total[i] is None else total[i] + term
                        else:
                            term = block_ref[i, c, 24:27, span] * near[0:3]
                            tail[i] = term if tail[i] is None else tail[i] + term
            for i in range(3):
                pulled[i, j : j + 1, :] = jnp.sum(total[i], axis=0, keepdims=True) + jnp.sum(
                    tail[i], axis=0, keepdims=True
                )
        return [right[i] - (diagonal[i] * field[i] - pulled[i]) for i in range(3)]

    def smooth(low, high):
        residual = apply_fine(low, high)
        values = [field[i] + damping * residual[i] / diagonal[i] for i in range(3)]
        for i in range(3):
            field[i] = values[i]
        return values

    wait_halo(0)
    send_halo(1, smooth(halo_in.at[0, 0], halo_in.at[0, 1]))
    wait_halo(1)
    residual = apply_fine(halo_in.at[1, 0], halo_in.at[1, 1])

    sums = [[zero] * 4 for _ in range(3)]
    for j in range(8):
        label = spread(label_ref[j : j + 1, :])
        for a in range(4):
            mine = label == sub + 8 * a
            for c in range(3):
                sums[c][a] = sums[c][a] + jnp.where(mine, spread(residual[c][j : j + 1, :]), 0.0)
    stacked = jnp.concatenate([part for line in sums for part in line] + [zero] * 4, axis=0)
    far_sums[block] = jnp.sum(stacked.T, axis=0, keepdims=True)
    send_far(far_sums.at[block], 1)

    wait_far(far_table, 0, far_recv)
    part = lanes >> 5
    for h in range(2):
        for k in range(4):
            rows = 32 * h + 8 * k
            for group in range(3):
                come = [far_table[4 * h + jj, 32 * group + 8 * k : 32 * group + 8 * k + 8, :] for jj in range(4)]
                for quarter in range(4):
                    q = 4 * group + quarter
                    if q > 9 and k > 0:
                        continue
                    value = None
                    for jj in range(4):
                        shift = (32 * (jj - quarter)) % LANES
                        moved = pltpu.roll(come[jj], shift, 1) if shift else come[jj]
                        value = moved if value is None else jnp.where(part == jj, moved, value)
                    if q < 9:
                        coarse_block[q, rows : rows + 8, :] = value
                    elif q == 9:
                        coarse_place[rows : rows + 8, :] = value.astype(jnp.int32)
                    elif q == 10:
                        tile[3 * h : 3 * h + 3, :] = value[0:3]
                    else:
                        tile[6 + h : 7 + h, :] = value[0:1]
    near_table[0, member] = tile[...]
    send_near(0)

    wait_far(far_sums, 1, far_recv)
    gathered = zero
    component = jnp.where(sub < 3, sub, sub - 3)
    lane = (jnp.where(sub < 6, component, 0) << 5) | (lanes & 31)
    for j in range(BLOCKS):
        mine = (part == j % 4) & (sub >= 3 * (j // 4)) & (sub < 3 * (j // 4) + 3)
        gathered = jnp.where(mine, pick(spread(far_sums[j]), lane), gathered)
    near_table[1, member] = gathered
    send_near(1)

    wait_near(0, near_recv)
    found = jnp.zeros((64, LANES), jnp.float32)
    high_id, low_id = iota((32, LANES), 0), iota((LANES, LANES), 0)
    lane_id = iota((32, LANES), 1)
    for m in range(MEMBERS):
        left, turn = [], []
        for h in range(2):
            where = near_table[0, m, 6 + h : 7 + h, :].astype(jnp.int32)
            hit = spread(where >> 7, (32, LANES)) == high_id
            left.append(
                jnp.concatenate(
                    [
                        jnp.where(hit, jnp.float32(2 * m + h), 0.0),
                        jnp.where(hit, lane_id.astype(jnp.float32), 0.0),
                    ],
                    axis=0,
                )
            )
            turn.append(jnp.where(spread(where & (LANES - 1), (LANES, LANES)) == low_id, 1.0, 0.0))
        found = found + lax.dot_general(
            jnp.concatenate(left, axis=1).astype(jnp.bfloat16),
            jnp.concatenate(turn, axis=1).astype(jnp.bfloat16),
            (((1,), (1,)), ((), ())),
            preferred_element_type=jnp.float32,
        )
    inverse_chunk[...] = found[0:32].astype(jnp.int32)
    inverse_lane[...] = found[32:64].astype(jnp.int32)

    wait_near(1, near_recv)
    near_sums = [near_table[1, m] for m in range(MEMBERS)]
    for m in range(MEMBERS):
        halves = []
        for h in range(2):
            row = 2 * m + h
            chunk = spread(inverse_chunk[row : row + 1, :])
            lane = spread(inverse_lane[row : row + 1, :])
            owner = chunk >> 1
            value = zero
            for n in range(MEMBERS):
                value = jnp.where(owner == n, pick(near_sums[n], lane), value)
            first, second = (value, pltpu.roll(value, 5, 0)) if h == 0 else (pltpu.roll(value, 3, 0), value)
            halves.append(jnp.where((chunk & 1) == 0, first, second))
        value = jnp.where(sub < 3, halves[0], jnp.where(sub < 6, halves[1], 0.0))
        rhs[m] = value
        near_table[2, m] = damping * value / jnp.where(sub < 6, near_table[0, m], 1.0)

    own_diagonal = jnp.where(sub < 6, near_table[0, member], 1.0)

    def source_row(step, chunk, c):
        at = 3 * (chunk % 2) + c
        return near_table[step, chunk // 2, at : at + 1, :]

    def coarse_sweep(step):
        for h in range(2):
            total = [zero] * 3
            for k in range(4):
                rows = 32 * h + 8 * k
                where = coarse_place[rows : rows + 8, :]
                lane, chunk = where & (LANES - 1), where >> 7
                near = [zero] * 3
                for n in range(2 * MEMBERS):
                    mine = chunk == n
                    for c in range(3):
                        near[c] = jnp.where(mine, pick(spread(source_row(step, n, c)), lane), near[c])
                for i in range(3):
                    for c in range(3):
                        total[i] = total[i] + coarse_block[3 * i + c, rows : rows + 8, :] * near[c]
            for i in range(3):
                tile[3 * h + i : 3 * h + i + 1, :] = jnp.sum(total[i], axis=0, keepdims=True)
        old = near_table[step, member]
        pull = jnp.where(sub < 6, tile[...], 0.0)
        return old + damping * (rhs[member] - (own_diagonal * old - pull)) / own_diagonal

    def sweep(step, carry):
        near_table[step + 1, member] = coarse_sweep(step)
        send_near(step + 1)
        wait_near(step + 1, near_recv)
        return carry

    lax.fori_loop(2, 2 + CSWEEPS - 1, sweep, 0)
    last = 1 + CSWEEPS

    mine = near_table[last, member]
    mine = jnp.where(block >= 4, pltpu.roll(mine, 5, 0), mine)
    quarter = block & 3
    shown = mine
    for jj in range(1, 4):
        shown = jnp.where(quarter == jj, pltpu.roll(mine, LANES - 32 * jj, 1), shown)
    correction_ref[...] = shown[0:3, 0:32]

    halo_place = [halo_in[0, 0, 6:8, :], halo_in[0, 1, 6:8, :]]
    where_own = node_place[...].astype(jnp.int32)
    halo_new[0, 0:2, :] = halo_place[0]
    halo_new[0, 2:4, :] = halo_place[1]
    halo_new[0, 4:8, :] = zero[0:4]
    where_halo = halo_new[0].astype(jnp.int32)
    lane_own, chunk_own = where_own & (LANES - 1), where_own >> 7
    lane_halo, chunk_halo = where_halo & (LANES - 1), where_halo >> 7
    add_own, add_halo = [zero] * 3, [zero] * 3
    for n in range(2 * MEMBERS):
        for c in range(3):
            source = spread(source_row(last, n, c))
            add_own[c] = jnp.where(chunk_own == n, pick(source, lane_own), add_own[c])
            add_halo[c] = jnp.where(chunk_halo == n, pick(source, lane_halo), add_halo[c])
    for c in range(3):
        field[c] = field[c] + add_own[c]
        halo_new[0, 2 * c : 2 * c + 2, :] = halo_in[1, 0, 2 * c : 2 * c + 2, :] + add_halo[c][0:2]
        halo_new[1, 2 * c : 2 * c + 2, :] = halo_in[1, 1, 2 * c : 2 * c + 2, :] + add_halo[c][2:4]

    send_halo(2, smooth(halo_new.at[0], halo_new.at[1]))
    wait_halo(2)
    values = smooth(halo_in.at[2, 0], halo_in.at[2, 1])
    for c in range(3):
        for j in range(8):
            out_ref[c : c + 1, j * LANES : (j + 1) * LANES] = values[c][j : j + 1]

    for step in range(3):
        for copy in halo_copies(step):
            copy.wait_send()
    wait_far(far_table, 0, far_send)
    wait_far(far_sums, 1, far_send)
    for step in range(2):
        wait_near(step, near_send)

    def drain(step, carry):
        wait_near(step, near_send)
        return carry

    lax.fori_loop(3, 2 + CSWEEPS, drain, 0)


def per_device(
    right_side,
    fine_diagonal,
    fine_columns,
    fine_blocks,
    aggregate_of_node,
    coarse_row_of_aggregate,
    coarse_diagonal,
    coarse_columns,
    coarse_blocks,
):
    nodes = right_side.shape[0]
    own = coarse_diagonal.shape[0]
    steps = 2 + CSWEEPS
    f32 = jnp.float32
    vmem = pl.BlockSpec(memory_space=pltpu.VMEM)
    field, correction = pl.pallas_call(
        kernel,
        out_shape=(jax.ShapeDtypeStruct((3, nodes), f32), jax.ShapeDtypeStruct((3, own), f32)),
        in_specs=[vmem] * 9,
        out_specs=(vmem, vmem),
        scratch_shapes=[
            pltpu.VMEM((3, 8, LANES), f32),
            pltpu.VMEM((3, 8, LANES), f32),
            pltpu.VMEM((32, nodes), jnp.int32),
            pltpu.VMEM((3, 8, LANES), f32),
            pltpu.VMEM((3, 8, LANES), f32),
            pltpu.VMEM((3, 2, 8, LANES), f32),
            pltpu.VMEM((3, 2, 8, LANES), f32),
            pltpu.VMEM((2, 8, LANES), f32),
            pltpu.VMEM((8, LANES), f32),
            pltpu.VMEM((384, LANES), f32),
            pltpu.VMEM((16, LANES), f32),
            pltpu.VMEM((BLOCKS, 96, LANES), f32),
            pltpu.VMEM((BLOCKS, 1, LANES), f32),
            pltpu.VMEM((steps, MEMBERS, 8, LANES), f32),
            pltpu.VMEM((9, 64, LANES), f32),
            pltpu.VMEM((64, LANES), jnp.int32),
            pltpu.VMEM((32, LANES), jnp.int32),
            pltpu.VMEM((32, LANES), jnp.int32),
            pltpu.VMEM((MEMBERS, 8, LANES), f32),
            pltpu.VMEM((8, LANES), f32),
            pltpu.SemaphoreType.DMA((3, 2)),
            pltpu.SemaphoreType.DMA((3, 2)),
            pltpu.SemaphoreType.DMA((2,)),
            pltpu.SemaphoreType.DMA((2,)),
            pltpu.SemaphoreType.DMA((steps,)),
            pltpu.SemaphoreType.DMA((steps,)),
        ],
        compiler_params=pltpu.CompilerParams(collective_id=0, has_side_effects=True),
    )(
        right_side.T,
        fine_diagonal.T,
        fine_columns.T,
        jnp.transpose(fine_blocks, (2, 3, 1, 0)),
        aggregate_of_node.reshape(8, LANES),
        coarse_row_of_aggregate.reshape(1, own),
        coarse_diagonal.T,
        coarse_columns,
        jnp.transpose(coarse_blocks, (2, 3, 0, 1)),
    )
    return (field.T, correction.T)


def solution(mesh):
    return jax.shard_map(
        per_device,
        mesh=mesh,
        in_specs=(
            P("dom", None),
            P("dom", None),
            P("dom", None),
            P("dom", None, None, None),
            P("dom"),
            P("dom"),
            P("dom", None),
            P("dom", None),
            P("dom", None, None, None),
        ),
        out_specs=(P("dom", None), P("dom", None)),
        check_vma=False,
    )
```

```python
import jax
import jax.numpy as jnp
from jax import lax
from jax.experimental import pallas as pl
from jax.experimental.pallas import tpu as pltpu
from jax.sharding import PartitionSpec as P

MESH = pl.DeviceIdType.MESH
LANES = 128
WIN = 256
CSWEEPS = 6
NEAR_BITS = (1, 2, 8, 32)
FAR_BITS = (4, 16, 64)
damping = 0.7


def subsets(bits):
    masks = [0]
    for bit in bits:
        masks = masks + [mask ^ bit for mask in masks]
    return sorted(masks[1:], key=lambda mask: -bin(mask).count("1"))


NEAR = subsets(NEAR_BITS)
FAR = subsets(FAR_BITS)
MEMBERS, BLOCKS = len(NEAR) + 1, len(FAR) + 1


def bit(value, position):
    return (value >> position) & 1


def member_of(device):
    return (device & 3) | (bit(device, 3) << 2) | (bit(device, 5) << 3)


def block_of(device):
    return bit(device, 2) | (bit(device, 4) << 1) | (bit(device, 6) << 2)


def place_of(row):
    device = row >> 5
    return (member_of(device) << 8) | (block_of(device) << 5) | (row & 31)


def pick(source, lane):
    return jnp.take_along_axis(source, lane, axis=1, mode="promise_in_bounds")


def spread(row, shape=(8, LANES)):
    return jnp.broadcast_to(row, shape)


def iota(shape, axis):
    return lax.broadcasted_iota(jnp.int32, shape, axis)


def kernel(
    right_hbm, diagonal_hbm, column_hbm, block_hbm, label_hbm, own_hbm, cdiagonal_hbm, ccolumn_hbm, cblock_hbm,
    out_ref, correction_ref,
    right_ref, diagonal_ref, column_ref, block_ref, label_ref, own_ref, cdiagonal_ref, ccolumn_ref, cblock_ref,
    right, diagonal, place, first, second, third, fourth, pulled, halo_out, halo_in, node_place, edge_out, edge_in,
    halo_block, halo_column,
    before, aside, far_table, far_sums, near_table, coarse_block, coarse_place, inverse_chunk, inverse_lane, rhs, tile,
    load_sem, halo_send, halo_recv, far_send, far_recv, near_send, near_recv,
):
    me = lax.axis_index("dom")
    devices = lax.axis_size("dom")
    member, block = member_of(me), block_of(me)
    after_me, before_me = lax.rem(me + 1, devices), lax.rem(me + devices - 1, devices)
    has_after, has_before = me < devices - 1, me > 0
    zero = jnp.zeros((8, LANES), jnp.float32)
    sub, lanes = iota((8, LANES), 0), iota((8, LANES), 1)

    barrier = pltpu.get_barrier_semaphore()

    def greet(device):
        pl.semaphore_signal(barrier, inc=1, device_id=(device,), device_id_type=MESH)

    for mask in FAR + NEAR:
        greet(me ^ mask)
    pl.when(has_after)(lambda: greet(after_me))
    pl.when(has_before)(lambda: greet(before_me))

    loads = [
        pltpu.make_async_copy(source, target, load_sem.at[index])
        for index, (source, target) in enumerate(
            [
                (right_hbm, right_ref),
                (diagonal_hbm, diagonal_ref),
                (column_hbm, column_ref),
                (block_hbm, block_ref),
                (label_hbm, label_ref),
                (own_hbm, own_ref),
                (cdiagonal_hbm, cdiagonal_ref),
                (ccolumn_hbm, ccolumn_ref),
                (cblock_hbm, cblock_ref),
            ]
        )
    ]
    for index in (0, 1, 4, 5, 2, 3, 8, 7, 6):
        loads[index].start()

    def remote(source, target, send, recv, device):
        return pltpu.make_async_remote_copy(
            src_ref=source, dst_ref=target, send_sem=send, recv_sem=recv, device_id=(device,), device_id_type=MESH
        )

    def halo_pair(step):
        if step == 0:
            sources = [halo_out.at[0], halo_out.at[1]]
            targets = [halo_in.at[0], halo_in.at[1]]
        elif step == 1:
            sources = [block_ref.at[:, :, :, 768:1024], block_ref.at[:, :, :, 0:256]]
            targets = [halo_block.at[0], halo_block.at[1]]
        elif step == 2:
            sources = [column_ref.at[:, 768:1024], column_ref.at[:, 0:256]]
            targets = [halo_column.at[0], halo_column.at[1]]
        else:
            sources = [edge_out.at[0], edge_out.at[1]]
            targets = [edge_in.at[0], edge_in.at[1]]
        return [
            remote(sources[d], targets[d], halo_send.at[step, d], halo_recv.at[step, d], device)
            for d, device in enumerate((after_me, before_me))
        ]

    def send_halo(step):
        ahead, back = halo_pair(step)
        pl.when(has_after)(ahead.start)
        pl.when(has_before)(back.start)

    def wait_halo(step):
        ahead, back = halo_pair(step)
        pl.when(has_before)(ahead.wait_recv)
        pl.when(has_after)(back.wait_recv)

    def close_halo(step):
        ahead, back = halo_pair(step)
        pl.when(has_after)(ahead.wait_send)
        pl.when(has_before)(back.wait_send)

    def send_near(step):
        own = near_table.at[step, member]
        for mask in NEAR:
            remote(own, own, near_send.at[step], near_recv.at[step], me ^ mask).start()

    def wait_near(step, sems):
        whole = near_table.at[step, pl.ds(0, MEMBERS - 1)]
        pltpu.make_async_copy(whole, whole, sems.at[step]).wait()

    def send_far(own, index):
        for mask in FAR:
            remote(own, own, far_send.at[index], far_recv.at[index], me ^ mask).start()

    def wait_far(table, index, sems):
        whole = table.at[pl.ds(0, BLOCKS - 1)]
        pltpu.make_async_copy(whole, whole, sems.at[index]).wait()

    def apply_fine(field, chunks):
        for j in chunks:
            if j < 0:
                matrix, span = halo_block.at[0], slice((j + 2) * LANES, (j + 3) * LANES)
            elif j < 8:
                matrix, span = block_ref, slice(j * LANES, (j + 1) * LANES)
            else:
                matrix, span = halo_block.at[1], slice((j - 8) * LANES, (j - 7) * LANES)
            here = slice((j + 2) * LANES, (j + 3) * LANES)
            source = [[field[c, j + t + 2 : j + t + 3, :] for t in range(5)] for c in range(3)]
            total = [None] * 3
            tail = [None] * 3
            for k in range(4):
                where = place[8 * k : 8 * k + 8, here]
                lane, chunk = where & (LANES - 1), where >> 7
                masks = [chunk == t for t in range(1, 5)]
                for c in range(3):
                    near = pick(spread(source[c][0]), lane)
                    for t in range(1, 5):
                        near = jnp.where(masks[t - 1], pick(spread(source[c][t]), lane), near)
                    for i in range(3):
                        if k < 3:
                            term = matrix[i, c, 8 * k : 8 * k + 8, span] * near
                            total[i] = term if total[i] is None else total[i] + term
                        else:
                            term = matrix[i, c, 24:27, span] * near[0:3]
                            tail[i] = term if tail[i] is None else tail[i] + term
            for i in range(3):
                pulled[i, j + 4 : j + 5, :] = jnp.sum(total[i], axis=0, keepdims=True) + jnp.sum(
                    tail[i], axis=0, keepdims=True
                )

    def residual_of(field, c, low, high):
        rows = slice(low + 4, high + 4)
        return right[c, rows, :] - (diagonal[c, rows, :] * field[c, rows, :] - pulled[c, rows, :])

    def smooth(field, target, low, high):
        rows = slice(low + 4, high + 4)
        for c in range(3):
            target[c, rows, :] = field[c, rows, :] + damping * residual_of(field, c, low, high) / diagonal[c, rows, :]

    def place_columns(source, chunks, offset):
        for j in chunks:
            span = slice((j - offset) * LANES, (j - offset + 1) * LANES)
            here = slice((j + 2) * LANES, (j + 3) * LANES)
            start = me * (8 * LANES) + (j * LANES - WIN)
            for k in range(4):
                rows = slice(8 * k, min(8 * k + 8, 27))
                place[rows, here] = source[rows, span] - start

    place[24:32, :] = jnp.zeros((8, 12 * LANES), jnp.int32)
    before[...] = jnp.zeros(before.shape, jnp.float32)
    aside[...] = jnp.zeros(aside.shape, jnp.float32)
    for index in (0, 1, 4, 5):
        loads[index].wait()
    for c in range(3):
        for j in range(8):
            span = slice(j * LANES, (j + 1) * LANES)
            right[c, j + 4 : j + 5, :] = right_ref[c : c + 1, span]
            diagonal[c, j + 4 : j + 5, :] = diagonal_ref[c : c + 1, span]
    aside[8:9, 0:32] = place_of(own_ref[...]).astype(jnp.float32)
    node_place[...] = pick(spread(aside[8:9, :]), label_ref[...])
    for c in range(3):
        first[c, 4:12, :] = damping * right[c, 4:12, :] / diagonal[c, 4:12, :]
        for d in range(2):
            rows = slice(8, 12) if d == 0 else slice(4, 8)
            halo_out[d, 4 * c : 4 * c + 4, :] = right[c, rows, :]
            halo_out[d, 12 + 4 * c : 16 + 4 * c, :] = diagonal[c, rows, :]
    halo_out[0, 24:28, :] = node_place[4:8, :]
    halo_out[1, 24:28, :] = node_place[0:4, :]
    halo_out[0, 28:32, :] = zero[0:4]
    halo_out[1, 28:32, :] = zero[0:4]

    loads[2].wait()
    place_columns(column_ref, range(8), 0)
    loads[3].wait()
    apply_fine(first, range(2, 6))
    smooth(first, second, 2, 6)
    for c in range(3):
        edge_out[0, 2 * c : 2 * c + 2, :] = second[c, 8:10, :]
        edge_out[1, 2 * c : 2 * c + 2, :] = second[c, 6:8, :]
    edge_out[0, 6:8, :] = zero[0:2]
    edge_out[1, 6:8, :] = zero[0:2]

    for index in (6, 7, 8):
        loads[index].wait()
    for i in range(3):
        for c in range(3):
            q = 3 * i + c
            before[32 * q : 32 * q + 32, 0:27] = cblock_ref[i, c]
    before[288:320, 0:27] = place_of(ccolumn_ref[...]).astype(jnp.float32)
    aside[0:3, 0:32] = cdiagonal_ref[...]
    own_block = far_table.at[block]
    for group in range(3):
        turned = before[128 * group : 128 * group + 128, :].T
        own_block[32 * group : 32 * group + 32, :] = turned[0:32, :]
    extra = pltpu.roll(aside[0:8, :], 64, 1) + pltpu.roll(aside[8:16, :], 96, 1)
    own_block[64:72, :] = own_block[64:72, :] + extra

    neighbours = has_after.astype(jnp.int32) + has_before.astype(jnp.int32)
    pl.semaphore_wait(barrier, len(FAR) + len(NEAR) + neighbours)
    for step in range(4):
        send_halo(step)

    wait_halo(0)
    for c in range(3):
        for d, rows in enumerate((slice(0, 4), slice(12, 16))):
            right[c, rows, :] = halo_in[d, 4 * c : 4 * c + 4, :]
            diagonal[c, rows, :] = halo_in[d, 12 + 4 * c : 16 + 4 * c, :]
            first[c, rows, :] = damping * right[c, rows, :] / diagonal[c, rows, :]
    apply_fine(first, (0, 1, 6, 7))
    smooth(first, second, 0, 2)
    smooth(first, second, 6, 8)
    apply_fine(second, range(2, 6))

    def add_up(sums, chunks):
        for j in chunks:
            label = spread(label_ref[j : j + 1, :])
            lines = [residual_of(second, c, j, j + 1) for c in range(3)]
            for a in range(4):
                mine = label == sub + 8 * a
                for c in range(3):
                    sums[c][a] = sums[c][a] + jnp.where(mine, spread(lines[c]), 0.0)

    sums = [[zero] * 4 for _ in range(3)]
    add_up(sums, range(2, 6))

    wait_halo(1)
    wait_halo(2)
    place_columns(halo_column.at[0], (-2, -1), -2)
    place_columns(halo_column.at[1], (8, 9), 8)
    apply_fine(first, (-2, -1, 8, 9))
    smooth(first, second, -2, 0)
    smooth(first, second, 8, 10)
    apply_fine(second, (0, 1, 6, 7))
    add_up(sums, (0, 1, 6, 7))
    stacked = jnp.concatenate([part for line in sums for part in line] + [zero] * 4, axis=0)
    far_sums[block] = jnp.sum(stacked.T, axis=0, keepdims=True)
    send_far(far_sums.at[block], 1)
    send_far(own_block, 0)

    wait_far(far_table, 0, far_recv)
    part = lanes >> 5
    for h in range(2):
        for k in range(4):
            rows = 32 * h + 8 * k
            for group in range(3):
                come = [far_table[4 * h + jj, 32 * group + 8 * k : 32 * group + 8 * k + 8, :] for jj in range(4)]
                for quarter in range(4):
                    q = 4 * group + quarter
                    if q > 9 and k > 0:
                        continue
                    value = None
                    for jj in range(4):
                        shift = (32 * (jj - quarter)) % LANES
                        moved = pltpu.roll(come[jj], shift, 1) if shift else come[jj]
                        value = moved if value is None else jnp.where(part == jj, moved, value)
                    if q < 9:
                        coarse_block[q, rows : rows + 8, :] = value
                    elif q == 9:
                        coarse_place[rows : rows + 8, :] = value.astype(jnp.int32)
                    elif q == 10:
                        tile[3 * h : 3 * h + 3, :] = value[0:3]
                    else:
                        tile[6 + h : 7 + h, :] = value[0:1]
    near_table[0, member] = tile[...]
    send_near(0)

    wait_far(far_sums, 1, far_recv)
    gathered = zero
    component = jnp.where(sub < 3, sub, sub - 3)
    lane = (jnp.where(sub < 6, component, 0) << 5) | (lanes & 31)
    for j in range(BLOCKS):
        mine = (part == j % 4) & (sub >= 3 * (j // 4)) & (sub < 3 * (j // 4) + 3)
        gathered = jnp.where(mine, pick(spread(far_sums[j]), lane), gathered)
    near_table[1, member] = gathered
    send_near(1)

    wait_near(0, near_recv)
    found = jnp.zeros((64, LANES), jnp.float32)
    high_id, low_id = iota((32, LANES), 0), iota((LANES, LANES), 0)
    lane_id = iota((32, LANES), 1)
    for m in range(MEMBERS):
        left, turn = [], []
        for h in range(2):
            where = near_table[0, m, 6 + h : 7 + h, :].astype(jnp.int32)
            hit = spread(where >> 7, (32, LANES)) == high_id
            left.append(
                jnp.concatenate(
                    [
                        jnp.where(hit, jnp.float32(2 * m + h), 0.0),
                        jnp.where(hit, lane_id.astype(jnp.float32), 0.0),
                    ],
                    axis=0,
                )
            )
            turn.append(jnp.where(spread(where & (LANES - 1), (LANES, LANES)) == low_id, 1.0, 0.0))
        found = found + lax.dot_general(
            jnp.concatenate(left, axis=1).astype(jnp.bfloat16),
            jnp.concatenate(turn, axis=1).astype(jnp.bfloat16),
            (((1,), (1,)), ((), ())),
            preferred_element_type=jnp.float32,
        )
    inverse_chunk[...] = found[0:32].astype(jnp.int32)
    inverse_lane[...] = found[32:64].astype(jnp.int32)

    wait_near(1, near_recv)
    near_sums = [near_table[1, m] for m in range(MEMBERS)]
    for m in range(MEMBERS):
        halves = []
        for h in range(2):
            row = 2 * m + h
            chunk = spread(inverse_chunk[row : row + 1, :])
            lane = spread(inverse_lane[row : row + 1, :])
            owner = chunk >> 1
            value = zero
            for n in range(MEMBERS):
                value = jnp.where(owner == n, pick(near_sums[n], lane), value)
            low, high = (value, pltpu.roll(value, 5, 0)) if h == 0 else (pltpu.roll(value, 3, 0), value)
            halves.append(jnp.where((chunk & 1) == 0, low, high))
        value = jnp.where(sub < 3, halves[0], jnp.where(sub < 6, halves[1], 0.0))
        rhs[m] = value
        near_table[2, m] = damping * value / jnp.where(sub < 6, near_table[0, m], 1.0)

    own_diagonal = jnp.where(sub < 6, near_table[0, member], 1.0)

    def source_row(step, chunk, c):
        at = 3 * (chunk % 2) + c
        return near_table[step, chunk // 2, at : at + 1, :]

    def coarse_sweep(step):
        for h in range(2):
            total = [zero] * 3
            for k in range(4):
                rows = 32 * h + 8 * k
                where = coarse_place[rows : rows + 8, :]
                lane, chunk = where & (LANES - 1), where >> 7
                near = [zero] * 3
                for n in range(2 * MEMBERS):
                    mine = chunk == n
                    for c in range(3):
                        near[c] = jnp.where(mine, pick(spread(source_row(step, n, c)), lane), near[c])
                for i in range(3):
                    for c in range(3):
                        total[i] = total[i] + coarse_block[3 * i + c, rows : rows + 8, :] * near[c]
            for i in range(3):
                tile[3 * h + i : 3 * h + i + 1, :] = jnp.sum(total[i], axis=0, keepdims=True)
        old = near_table[step, member]
        pull = jnp.where(sub < 6, tile[...], 0.0)
        return old + damping * (rhs[member] - (own_diagonal * old - pull)) / own_diagonal

    def sweep(step, carry):
        near_table[step + 1, member] = coarse_sweep(step)
        send_near(step + 1)
        wait_near(step + 1, near_recv)
        return carry

    lax.fori_loop(2, 2 + CSWEEPS - 1, sweep, 0)
    last = 1 + CSWEEPS

    mine = near_table[last, member]
    mine = jnp.where(block >= 4, pltpu.roll(mine, 5, 0), mine)
    quarter = block & 3
    shown = mine
    for jj in range(1, 4):
        shown = jnp.where(quarter == jj, pltpu.roll(mine, LANES - 32 * jj, 1), shown)
    correction_ref[...] = shown[0:3, 0:32]

    where_own = node_place[...].astype(jnp.int32)
    where_halo = jnp.concatenate([halo_in[0, 24:28, :], halo_in[1, 24:28, :]], axis=0).astype(jnp.int32)
    lane_own, chunk_own = where_own & (LANES - 1), where_own >> 7
    lane_halo, chunk_halo = where_halo & (LANES - 1), where_halo >> 7
    add_own, add_halo = [zero] * 3, [zero] * 3
    for n in range(2 * MEMBERS):
        for c in range(3):
            source = spread(source_row(last, n, c))
            add_own[c] = jnp.where(chunk_own == n, pick(source, lane_own), add_own[c])
            add_halo[c] = jnp.where(chunk_halo == n, pick(source, lane_halo), add_halo[c])
    wait_halo(3)
    for c in range(3):
        second[c, 0:2, :] = edge_in[0, 2 * c : 2 * c + 2, :]
        second[c, 14:16, :] = edge_in[1, 2 * c : 2 * c + 2, :]
        third[c, 4:12, :] = second[c, 4:12, :] + add_own[c]
        third[c, 0:4, :] = second[c, 0:4, :] + add_halo[c][0:4]
        third[c, 12:16, :] = second[c, 12:16, :] + add_halo[c][4:8]

    apply_fine(third, range(-2, 10))
    smooth(third, fourth, -2, 10)
    apply_fine(fourth, range(8))
    for c in range(3):
        value = fourth[c, 4:12, :] + damping * residual_of(fourth, c, 0, 8) / diagonal[c, 4:12, :]
        for j in range(8):
            out_ref[c : c + 1, j * LANES : (j + 1) * LANES] = value[j : j + 1]

    for step in range(4):
        close_halo(step)
    wait_far(far_table, 0, far_send)
    wait_far(far_sums, 1, far_send)
    for step in range(2):
        wait_near(step, near_send)

    def drain(step, carry):
        wait_near(step, near_send)
        return carry

    lax.fori_loop(3, 2 + CSWEEPS, drain, 0)


def finish(field_ref, correction_ref, out_field_ref, out_correction_ref):
    out_field_ref[...] = field_ref[...]
    out_correction_ref[...] = correction_ref[...]


def per_device(
    right_side,
    fine_diagonal,
    fine_columns,
    fine_blocks,
    aggregate_of_node,
    coarse_row_of_aggregate,
    coarse_diagonal,
    coarse_columns,
    coarse_blocks,
):
    nodes = right_side.shape[0]
    own = coarse_diagonal.shape[0]
    steps = 2 + CSWEEPS
    f32 = jnp.float32
    i32 = jnp.int32
    vmem = pl.BlockSpec(memory_space=pltpu.VMEM)
    anywhere = pl.BlockSpec(memory_space=pl.ANY)
    shapes = (jax.ShapeDtypeStruct((3, nodes), f32), jax.ShapeDtypeStruct((3, own), f32))
    operands = (
        right_side.T,
        fine_diagonal.T,
        fine_columns.T,
        jnp.transpose(fine_blocks, (2, 3, 1, 0)),
        aggregate_of_node.reshape(8, LANES),
        coarse_row_of_aggregate.reshape(1, own),
        coarse_diagonal.T,
        coarse_columns,
        jnp.transpose(coarse_blocks, (2, 3, 0, 1)),
    )
    tall = pltpu.VMEM((3, 16, LANES), f32)
    outs = pl.pallas_call(
        kernel,
        out_shape=shapes,
        in_specs=[anywhere] * 9,
        out_specs=(vmem, vmem),
        scratch_shapes=[pltpu.VMEM(operand.shape, operand.dtype) for operand in operands]
        + [
            tall,
            tall,
            pltpu.VMEM((32, 12 * LANES), i32),
            tall,
            tall,
            tall,
            tall,
            tall,
            pltpu.VMEM((2, 32, LANES), f32),
            pltpu.VMEM((2, 32, LANES), f32),
            pltpu.VMEM((8, LANES), f32),
            pltpu.VMEM((2, 8, LANES), f32),
            pltpu.VMEM((2, 8, LANES), f32),
            pltpu.VMEM((2, 3, 3, 27, WIN), f32),
            pltpu.VMEM((2, 27, WIN), i32),
            pltpu.VMEM((384, LANES), f32),
            pltpu.VMEM((16, LANES), f32),
            pltpu.VMEM((BLOCKS, 96, LANES), f32),
            pltpu.VMEM((BLOCKS, 1, LANES), f32),
            pltpu.VMEM((steps, MEMBERS, 8, LANES), f32),
            pltpu.VMEM((9, 64, LANES), f32),
            pltpu.VMEM((64, LANES), i32),
            pltpu.VMEM((32, LANES), i32),
            pltpu.VMEM((32, LANES), i32),
            pltpu.VMEM((MEMBERS, 8, LANES), f32),
            pltpu.VMEM((8, LANES), f32),
            pltpu.SemaphoreType.DMA((9,)),
            pltpu.SemaphoreType.DMA((4, 2)),
            pltpu.SemaphoreType.DMA((4, 2)),
            pltpu.SemaphoreType.DMA((2,)),
            pltpu.SemaphoreType.DMA((2,)),
            pltpu.SemaphoreType.DMA((steps,)),
            pltpu.SemaphoreType.DMA((steps,)),
        ],
        compiler_params=pltpu.CompilerParams(collective_id=0, has_side_effects=True),
    )(*operands)
    field, correction = pl.pallas_call(finish, out_shape=shapes, in_specs=[vmem] * 2, out_specs=(vmem, vmem))(*outs)
    return (field.T, correction.T)


def solution(mesh):
    return jax.shard_map(
        per_device,
        mesh=mesh,
        in_specs=(
            P("dom", None),
            P("dom", None),
            P("dom", None),
            P("dom", None, None, None),
            P("dom"),
            P("dom"),
            P("dom", None),
            P("dom", None),
            P("dom", None, None, None),
        ),
        out_specs=(P("dom", None), P("dom", None)),
        check_vma=False,
    )
```
